32 devices in a mesh: pole: 2 (over y), row: 8 (over z, x), col: 2 (over core).
Axes of the slice: x: 2, y: 2, z: 4, core: 2. Of those that a mesh axis runs over, the one named last changes fastest.
Arguments:
- known_inverse: float32 [16, 128, 1024], P('pole', 'col', 'row'), parts along dimension 0, may hold values from -1 to 3, as said below
- first_factor: float32 [2048, 512], P(('pole', 'row')), parts along dimension 0, may hold values from -0.5 to 0.5
- first_corner: float32 [1024, 512], P('pole'), parts along dimension 0, may hold values from -1 to 5, as said below
- first_ancestors: int32 [1024], P('pole'), parts along dimension 0, may hold values from 0 to 1023, as said below
- second_factor: float32 [2048, 512], P(('pole', 'row')), parts along dimension 0, may hold values from -0.75 to 0.75
- second_link: float32 [1024, 512], P('pole'), parts along dimension 0, may hold values from -0.25 to 0.25
- second_corner: float32 [1024, 512], P('pole', 'col'), parts along dimension 0, may hold values from -1 to 5, as said below
- second_ancestors: int32 [512], P('pole'), parts along dimension 0, may hold values from 0 to 1023, as said below
Outputs:
- first_column: float32 [2048, 512], P(('pole', 'row'), 'col'), parts along dimension 0
- first_diagonal: float32 [1024, 512], P('pole', 'col'), parts along dimension 0
- second_column: float32 [2048, 512], P(('pole', 'row'), 'col'), parts along dimension 0
- second_cross: float32 [1024, 512], P('pole', 'col'), parts along dimension 0
- second_diagonal: float32 [1024, 512], P('pole', 'col'), parts along dimension 0
The draws below stay inside these ranges and needn't reach their ends.
There are 2 independent parts, one for each index of `pole`. The reference program is written for one: setup_inputs(seed, part) draws one part's arguments, and reference() takes and returns one part's arrays. A program takes and returns all parts, laid end to end along the dimension named above; each array names one. Nothing has to cross between parts.
Inputs may be any that keep to these rules, and one draw needn't show every extreme that they name: `known_inverse`: K is symmetric. `first_corner`: symmetric. `second_corner`: symmetric. `first_ancestors`: distinct row numbers; every block of 128 consecutive row numbers starting at a multiple of 128 holds at least one of them. `second_ancestors`: distinct row numbers, each of which is also in first_ancestors; every block of 128 consecutive row numbers starting at a multiple of 128 holds at least one of them.
All inputs are finite; a program needn't handle non-finite values.
Results may differ from the reference program's by a relative error of at most 0.000084.
Values sent between devices are 32-bit elements; how exact they have to be, the bound alone decides.
A program may use at most 128 MiB of HBM per device.

```python
import jax
import jax.numpy as jnp
from jax import lax

BLOCK_ROWS = 128
WIDTH = 512
ANC_ROWS = 1024
FIRST_ANC = 512
SECOND_ANC = 256
N_ROW = 8


def symmetric_draw(key, order, lowest, highest, spread):
    noise_key, middle_key = jax.random.split(key)
    noise = jnp.clip(jax.random.normal(noise_key, (order, order), jnp.float32), -4.0, 4.0) * (spread / order ** 0.5)
    middle = jax.random.uniform(middle_key, (order,), jnp.float32, lowest, highest)
    return (noise + noise.T) * 0.5 + jnp.diag(middle)


def draw_known_inverse(key, part):
    whole = symmetric_draw(jax.random.fold_in(key, 3), ANC_ROWS, 0.5, 2.0, 0.5)
    return whole.reshape(N_ROW, BLOCK_ROWS, ANC_ROWS)


def draw_first_corner(key, part):
    return symmetric_draw(jax.random.fold_in(key, 5), WIDTH, 1.0, 3.0, 0.5)


def draw_second_corner(key, part):
    return symmetric_draw(jax.random.fold_in(key, 7), WIDTH, 1.0, 3.0, 0.5)


def ancestor_sets(key):
    numbers = jnp.arange(ANC_ROWS, dtype=jnp.int32)
    places = jax.random.randint(jax.random.fold_in(key, 20), (N_ROW,), 0, BLOCK_ROWS, dtype=jnp.int32)
    keeper = (numbers % BLOCK_ROWS == places[numbers // BLOCK_ROWS]).astype(jnp.int32)
    scores = keeper * ANC_ROWS + jax.random.randint(jax.random.fold_in(key, 21), (ANC_ROWS,), 0, ANC_ROWS, dtype=jnp.int32)
    chosen = jnp.sort(lax.top_k(scores * ANC_ROWS + numbers, FIRST_ANC)[1]).astype(jnp.int32)
    inner = jnp.arange(FIRST_ANC, dtype=jnp.int32)
    inner_scores = keeper[chosen] * ANC_ROWS + jax.random.randint(jax.random.fold_in(key, 22), (FIRST_ANC,), 0, ANC_ROWS, dtype=jnp.int32)
    subset = jnp.sort(chosen[lax.top_k(inner_scores * FIRST_ANC + inner, SECOND_ANC)[1]]).astype(jnp.int32)
    return (chosen, subset)


def draw_first_ancestors(key, part):
    return ancestor_sets(key)[0]


def draw_second_ancestors(key, part):
    return ancestor_sets(key)[1]


def levels(own_key, shape, pieces, least, high):
    gain, own = 1.0, jax.random.fold_in(own_key, 6)
    for axis_at, parts in pieces:
        draws = jnp.exp(jax.random.uniform(jax.random.fold_in(own, axis_at), (parts,), jnp.float32, least / len(pieces), high / len(pieces)))
        gain = gain * jnp.repeat(draws, shape[axis_at] // parts).reshape([-1 if axis == axis_at else 1 for axis in range(len(shape))])
    return gain


def bell_draw(own_key, extent, scale, most, shards=(), kind=jnp.bfloat16):
    array = scale * jax.random.normal(own_key, extent, jnp.float32)
    if shards:
        array = array * levels(own_key, extent, shards, -0.22, 0.18)
    return jnp.clip(array, -most, most).astype(kind)


def setup_inputs(seed: int = 0, part: int = 0) -> dict:
    key_of = jax.random.split(jax.random.key(seed), 9)
    part_keys = jax.random.split(jax.random.fold_in(key_of[8], part), 9)
    known_inverse = draw_known_inverse(jax.random.fold_in(jax.random.fold_in(key_of[8], part), 71), part)
    first_factor = bell_draw(part_keys[1], (ANC_ROWS, WIDTH), (FIRST_ANC // 4) ** -0.5, 0.5, ((0, 8),), jnp.float32)
    first_corner = draw_first_corner(jax.random.fold_in(jax.random.fold_in(key_of[8], part), 71), part)
    first_ancestors = draw_first_ancestors(jax.random.fold_in(jax.random.fold_in(key_of[8], part), 71), part)
    second_factor = bell_draw(part_keys[4], (ANC_ROWS, WIDTH), (SECOND_ANC // 4) ** -0.5, 0.75, ((0, 8),), jnp.float32)
    second_link = bell_draw(part_keys[5], (WIDTH, WIDTH), WIDTH ** -0.5, 0.25, (), jnp.float32)
    second_corner = draw_second_corner(jax.random.fold_in(jax.random.fold_in(key_of[8], part), 71), part)
    second_ancestors = draw_second_ancestors(jax.random.fold_in(jax.random.fold_in(key_of[8], part), 71), part)
    return {"known_inverse": known_inverse, "first_factor": first_factor, "first_corner": first_corner, "first_ancestors": first_ancestors, "second_factor": second_factor, "second_link": second_link, "second_corner": second_corner, "second_ancestors": second_ancestors}


HIGH = lax.Precision.HIGHEST


def product(left, right):
    return jnp.dot(left, right, precision=HIGH, preferred_element_type=jnp.float32)


def transposed_product(left, right):
    return lax.dot_general(left, right, (((0,), (0,)), ((), ())), precision=HIGH, preferred_element_type=jnp.float32)


def row_mask(ancestors):
    return jnp.zeros((ANC_ROWS,), jnp.float32).at[ancestors].set(1.0)[:, None]


def reference(known_inverse, first_factor, first_corner, first_ancestors, second_factor, second_link, second_corner, second_ancestors):
    columns = known_inverse.reshape(ANC_ROWS, ANC_ROWS)
    first_mask = row_mask(first_ancestors)
    second_mask = row_mask(second_ancestors)
    first_masked = first_factor * first_mask
    second_masked = second_factor * second_mask
    first_column = -(transposed_product(columns, first_masked) * first_mask)
    first_diagonal = first_corner - transposed_product(first_masked, first_column)
    second_column = -((transposed_product(columns, second_masked) + product(first_column, second_link)) * second_mask)
    second_cross = -(transposed_product(first_column, second_masked) + product(first_diagonal, second_link))
    second_diagonal = second_corner - transposed_product(second_masked, second_column) - transposed_product(second_link, second_cross)
    return (first_column, first_diagonal, second_column, second_cross, second_diagonal)
```

```python
import functools

import jax
import jax.numpy as jnp
from jax import lax
from jax.experimental import pallas as pl
from jax.experimental.pallas import tpu as pltpu
from jax.sharding import PartitionSpec as P

HIGH = lax.Precision.HIGHEST
MESH = pl.DeviceIdType.MESH
LANES_OF_RING = 2
VMEM_FOR_WHOLE = 40 * 2**20


def product(left, right):
    return jnp.dot(left, right, precision=HIGH, preferred_element_type=jnp.float32)


def transposed_product(left, right):
    return lax.dot_general(
        left, right, (((0,), (0,)), ((), ())), precision=HIGH, preferred_element_type=jnp.float32
    )


def local_mask(ancestors, row_start, block_rows):
    global_rows = row_start + jnp.arange(block_rows, dtype=jnp.int32)
    return jnp.any(ancestors[:, None] == global_rows[None, :], axis=0).astype(jnp.float32)[:, None]


def on_device_collectives(
    known_inverse,
    first_factor,
    first_corner,
    first_ancestors,
    second_factor,
    second_link,
    second_corner,
    second_ancestors,
):
    groups, share_rows, block_rows = known_inverse.shape
    half_width = second_corner.shape[1]
    col_index = lax.axis_index("col")
    row_start = lax.axis_index("row") * block_rows
    first_mask = local_mask(first_ancestors, row_start, block_rows)
    second_mask = local_mask(second_ancestors, row_start, block_rows)
    first_masked = first_factor * first_mask
    second_masked = second_factor * second_mask
    share_start = col_index * share_rows
    first_piece = lax.dynamic_slice_in_dim(first_masked, share_start, share_rows, 0)
    second_piece = lax.dynamic_slice_in_dim(second_masked, share_start, share_rows, 0)
    columns = known_inverse.reshape(groups * share_rows, block_rows)

    def add_piece(piece):
        return transposed_product(columns, piece)

    first_partial = add_piece(lax.all_gather(first_piece, "row", axis=0, tiled=True))
    second_partial = add_piece(lax.all_gather(second_piece, "row", axis=0, tiled=True))
    first_image = lax.psum_scatter(first_partial, "col", scatter_dimension=1, tiled=True)
    first_column = -(first_image * first_mask)
    first_full = lax.all_gather(first_column, "col", axis=1, tiled=True)
    diagonal_partial = transposed_product(first_masked, first_column)
    corner_half = lax.dynamic_slice_in_dim(first_corner, col_index * half_width, half_width, 1)
    first_diagonal = corner_half - lax.psum(diagonal_partial, "row")
    diagonal_full = lax.all_gather(first_diagonal, "col", axis=1, tiled=True)
    second_image = lax.psum_scatter(second_partial, "col", scatter_dimension=1, tiled=True)
    link_half = lax.dynamic_slice_in_dim(second_link, col_index * half_width, half_width, 1)
    second_column = -((second_image + product(first_full, link_half)) * second_mask)
    second_half = lax.dynamic_slice_in_dim(second_masked, col_index * half_width, half_width, 1)
    cross_partial = transposed_product(first_full, second_half)
    closing_partial = transposed_product(second_masked, second_column)
    cross_total, closing_total = lax.psum((cross_partial, closing_partial), "row")
    second_cross = -(cross_total + product(diagonal_full, link_half))
    second_diagonal = second_corner - closing_total - transposed_product(second_link, second_cross)
    return (first_column, first_diagonal, second_column, second_cross, second_diagonal)


def split(value):
    high = value.astype(jnp.bfloat16)
    return high, (value - high.astype(jnp.float32)).astype(jnp.bfloat16)


def dot(left, right):
    return jnp.dot(left, right, preferred_element_type=jnp.float32)


def dot3(left, right):
    (left_high, left_low), (right_high, right_low) = left, right
    return dot(left_high, right_high) + (dot(left_low, right_high) + dot(left_high, right_low))


def ring_kernel(
    n,
    known,
    factor_one,
    corner_one,
    ancestors_one,
    factor_two,
    link,
    corner_two,
    ancestors_two,
    column_one,
    diagonal_one,
    column_two,
    cross_two,
    diagonal_two,
    k_raw,
    f_raw,
    f_high,
    f_low,
    t_buf,
    own,
    link_buf,
    corner_buf,
    link_half,
    corner_half,
    corner_two_buf,
    link_split,
    half_split,
    local_sem,
    ring_send,
    ring_recv,
    pair_send,
    pair_recv,
):
    half = n // 2
    blocks = half + 1
    share = k_raw.shape[3]
    block = 2 * share
    width = link_buf.shape[0]
    hw = width // 2
    me_row = lax.axis_index("row")
    me_col = lax.axis_index("col")
    other_col = 1 - me_col

    length = n // LANES_OF_RING

    def row_at(position):
        position = lax.rem(position + n, n)
        lane = position // length
        step = position + lane * (2 * length - 1 - 2 * position)
        return step * LANES_OF_RING + lane

    lane = lax.rem(me_row, LANES_OF_RING)
    step = me_row // LANES_OF_RING
    place = step + lane * (2 * length - 1 - 2 * step)
    targets = (row_at(place + 1), row_at(place - 1))

    barrier = pltpu.get_barrier_semaphore()
    for target in targets:
        pl.semaphore_signal(barrier, inc=1, device_id={"row": target}, device_id_type=MESH)
    pl.semaphore_signal(barrier, inc=1, device_id={"col": other_col}, device_id_type=MESH)

    count = [0]

    def local(src, dst):
        copy = pltpu.make_async_copy(src, dst, local_sem.at[count[0]])
        count[0] += 1
        copy.start()
        return copy

    f_one = [local(factor_one.at[pl.ds(h * share, share)], f_raw.at[0, h, 0]) for h in range(2)]
    f_two = [local(factor_two.at[pl.ds(h * share, share)], f_raw.at[0, h, 1]) for h in range(2)]
    k_own = [local(known.at[row_at(place + i)], k_raw.at[0, me_col, i]) for i in range(blocks)]
    my_columns = pl.ds(pl.multiple_of(me_col * hw, 128), hw)
    rest = [
        local(link, link_buf),
        local(corner_one, corner_buf),
        local(link.at[:, my_columns], link_half),
        local(corner_one.at[:, my_columns], corner_half),
        local(corner_two, corner_two_buf),
    ]

    def slot(direction, t):
        return 0 if t == 0 else n - 1 if t == half else 2 * t - 1 + direction

    offsets = [0] * n
    for t in range(1, half):
        offsets[slot(0, t)], offsets[slot(1, t)] = -t, t
    offsets[n - 1] = half
    cut = half // 2

    def view(piece, at, which):
        if piece < 2:
            return f_raw.at[at, which, piece]
        if piece == 2:
            return k_raw.at[at, which]
        if piece == 3:
            return k_raw.at[at, which, pl.ds(0, cut)]
        return k_raw.at[at, which, pl.ds(cut, blocks - cut)]

    def pieces(direction, t):
        if t < half:
            return (0, 1, 2)
        return (0, 3) if direction == 0 else (1, 4)

    def ring(direction, t, piece):
        return pltpu.make_async_remote_copy(
            src_ref=view(piece, slot(direction, t - 1), me_col),
            dst_ref=view(piece, slot(direction, t), me_col),
            send_sem=ring_send.at[direction, t - 1, piece],
            recv_sem=ring_recv.at[direction, t - 1, piece],
            device_id={"row": targets[direction]},
            device_id_type=MESH,
        )

    def pair(at, piece, which):
        return pltpu.make_async_remote_copy(
            src_ref=view(piece, at, which),
            dst_ref=view(piece, at, which),
            send_sem=pair_send.at[at, piece],
            recv_sem=pair_recv.at[at, piece],
            device_id={"col": other_col},
            device_id_type=MESH,
        )

    sent = []

    def go(copy):
        copy.start()
        sent.append(copy)

    pl.semaphore_wait(barrier, 3)
    for piece, waits in ((0, f_one), (1, f_two), (2, k_own)):
        for copy in waits:
            copy.wait()
        for direction in range(2):
            go(ring(direction, 1, piece))
    go(pair(0, 2, me_col))

    for copy in rest:
        copy.wait()
    link_split[0], link_split[1] = split(link_buf[...])
    half_split[0], half_split[1] = split(link_half[...])
    corner_link = dot3(split(corner_buf[...]), (half_split[0], half_split[1]))
    cross_two[...] = -corner_link
    diagonal_one[...] = corner_half[...]
    diagonal_two[...] = corner_two_buf[...] + dot3(split(link_buf[...].T), split(corner_link))
    own[...] = jnp.zeros_like(own)

    def mask_of(ancestors, row_start):
        rows = row_start + lax.broadcasted_iota(jnp.int32, (block, ancestors.shape[1]), 0)
        same = jnp.where(rows == ancestors[...], 1.0, 0.0)
        return jnp.max(same, axis=1, keepdims=True)

    def k_block(a, b):
        i = (offsets[a] - offsets[b]) % n
        if i <= half:
            return k_raw[b, :, i].reshape(block, block)
        return k_raw[a, :, n - i].reshape(block, block).T

    def mine(ref, start):
        return ref[:, pl.ds(pl.multiple_of(start + me_col * hw, 128), hw)]

    def process(k):
        row_start = row_at(place + offsets[k]) * block
        first = f_raw[k, :, 0].reshape(block, width) * mask_of(ancestors_one, row_start)
        second = f_raw[k, :, 1].reshape(block, width) * mask_of(ancestors_two, row_start)
        reduced = second - dot3(split(first), (link_split[0], link_split[1]))
        rows = pl.ds(k * block, block)
        both = jnp.concatenate([first, reduced], axis=1)
        f_high[rows, :], f_low[rows, :] = split(both)
        my_high = jnp.concatenate([mine(f_high.at[rows], 0), mine(f_high.at[rows], width)], axis=1)
        my_low = jnp.concatenate([mine(f_low.at[rows], 0), mine(f_low.at[rows], width)], axis=1)
        own[...] += dot3(split(k_block(0, k)), (my_high, my_low))
        diagonal_part = dot3(split(k_block(k, k)), (my_high, my_low))
        if k == 0:
            left = both.T
            right_high, right_low = split(diagonal_part)
        else:
            past = pl.ds(0, k * block)
            line_high, line_low = split(jnp.concatenate([k_block(k, j) for j in range(k)], axis=1))
            image = dot3((line_high, line_low), (f_high[past, :], f_low[past, :]))
            t_buf[...] = image
            left = jnp.concatenate([both.T, image.T], axis=1)
            image_mine = jnp.concatenate([mine(t_buf, 0), mine(t_buf, width)], axis=1)
            image_high, image_low = split(image_mine + diagonal_part)
            right_high = jnp.concatenate([image_high, my_high], axis=0)
            right_low = jnp.concatenate([image_low, my_low], axis=0)
        left_high, left_low = split(left)
        add = dot3((left_high[:width], left_low[:width]), (right_high, right_low))
        diagonal_one[...] += add[:, :hw]
        cross_two[...] += add[:, hw:]
        diagonal_two[...] += dot3((left_high[width:], left_low[width:]), (right_high[:, hw:], right_low[:, hw:]))

    pair(0, 2, other_col).wait_recv()
    process(0)
    for t in range(1, half):
        for piece in range(3):
            for direction in range(2):
                ring(direction, t, piece).wait_recv()
                for later in pieces(direction, t + 1):
                    if later == piece or (piece == 2 and later > 2):
                        go(ring(direction, t + 1, later))
                go(pair(slot(direction, t), piece, me_col))
        for direction in range(2):
            for piece in range(3):
                pair(slot(direction, t), piece, other_col).wait_recv()
            process(slot(direction, t))
    last = [(direction, pieces(direction, half)[i]) for i in range(2) for direction in range(2)]
    for direction, piece in last:
        ring(direction, half, piece).wait_recv()
        go(pair(n - 1, piece, me_col))
    for direction, piece in last:
        pair(n - 1, piece, other_col).wait_recv()
    process(n - 1)
    first_rows = mask_of(ancestors_one, me_row * block)
    second_rows = mask_of(ancestors_two, me_row * block)
    column_one[...] = -(own[:, :hw] * first_rows)
    column_two[...] = -(own[:, hw:] * second_rows)
    for copy in sent:
        copy.wait_send()


def on_device_ring(
    n,
    known_inverse,
    first_factor,
    first_corner,
    first_ancestors,
    second_factor,
    second_link,
    second_corner,
    second_ancestors,
):
    groups, share, block = known_inverse.shape
    width = second_link.shape[0]
    hw = second_corner.shape[1]
    f32, bf16 = jnp.float32, jnp.bfloat16
    blocks = n // 2 + 1
    anywhere = pl.BlockSpec(memory_space=pl.ANY)
    vmem = pl.BlockSpec(memory_space=pltpu.VMEM)
    square = jax.ShapeDtypeStruct((width, hw), f32)
    column = jax.ShapeDtypeStruct((block, hw), f32)
    return pl.pallas_call(
        functools.partial(ring_kernel, n),
        out_shape=(column, square, column, square, square),
        in_specs=[anywhere, anywhere, anywhere, vmem, anywhere, anywhere, anywhere, vmem],
        out_specs=(vmem,) * 5,
        scratch_shapes=[
            pltpu.VMEM((n, 2, blocks, share, block), f32),
            pltpu.VMEM((n, 2, 2, share, width), f32),
            pltpu.VMEM((n * block, 2 * width), bf16),
            pltpu.VMEM((n * block, 2 * width), bf16),
            pltpu.VMEM((block, 2 * width), f32),
            pltpu.VMEM((block, width), f32),
            pltpu.VMEM((width, width), f32),
            pltpu.VMEM((width, width), f32),
            pltpu.VMEM((width, hw), f32),
            pltpu.VMEM((width, hw), f32),
            pltpu.VMEM((width, hw), f32),
            pltpu.VMEM((2, width, width), bf16),
            pltpu.VMEM((2, width, hw), bf16),
            pltpu.SemaphoreType.DMA((9 + blocks,)),
            pltpu.SemaphoreType.DMA((2, n // 2, 5)),
            pltpu.SemaphoreType.DMA((2, n // 2, 5)),
            pltpu.SemaphoreType.DMA((n, 5)),
            pltpu.SemaphoreType.DMA((n, 5)),
        ],
        compiler_params=pltpu.CompilerParams(collective_id=0, has_side_effects=True),
    )(
        known_inverse,
        first_factor,
        first_corner,
        first_ancestors.reshape(1, -1),
        second_factor,
        second_link,
        second_corner,
        second_ancestors.reshape(1, -1),
    )


def solution(mesh):
    def on_device(*args):
        n = mesh.shape["row"]
        groups, share, block = args[0].shape
        width = args[5].shape[0]
        held = 4 * n * block * (n * block + 4 * width)
        fits = (
            mesh.shape["col"] == 2
            and n % 4 == 0
            and groups == n
            and block == 2 * share
            and held <= VMEM_FOR_WHOLE
        )
        return on_device_ring(n, *args) if fits else on_device_collectives(*args)

    return jax.shard_map(
        on_device,
        mesh=mesh,
        in_specs=(
            P("pole", "col", "row"),
            P(("pole", "row"), None),
            P("pole", None),
            P("pole"),
            P(("pole", "row"), None),
            P("pole", None),
            P("pole", "col"),
            P("pole"),
        ),
        out_specs=(
            P(("pole", "row"), "col"),
            P("pole", "col"),
            P(("pole", "row"), "col"),
            P("pole", "col"),
            P("pole", "col"),
        ),
        check_vma=False,
    )
```

```python
import functools

import jax
import jax.numpy as jnp
from jax import lax
from jax.experimental import pallas as pl
from jax.experimental.pallas import tpu as pltpu
from jax.sharding import PartitionSpec as P

HIGH = lax.Precision.HIGHEST
MESH = pl.DeviceIdType.MESH
LANES_OF_RING = 2
VMEM_FOR_WHOLE = 40 * 2**20


def product(left, right):
    return jnp.dot(left, right, precision=HIGH, preferred_element_type=jnp.float32)


def transposed_product(left, right):
    return lax.dot_general(
        left, right, (((0,), (0,)), ((), ())), precision=HIGH, preferred_element_type=jnp.float32
    )


def local_mask(ancestors, row_start, block_rows):
    global_rows = row_start + jnp.arange(block_rows, dtype=jnp.int32)
    return jnp.any(ancestors[:, None] == global_rows[None, :], axis=0).astype(jnp.float32)[:, None]


def on_device_collectives(
    known_inverse,
    first_factor,
    first_corner,
    first_ancestors,
    second_factor,
    second_link,
    second_corner,
    second_ancestors,
):
    groups, share_rows, block_rows = known_inverse.shape
    half_width = second_corner.shape[1]
    col_index = lax.axis_index("col")
    row_start = lax.axis_index("row") * block_rows
    first_mask = local_mask(first_ancestors, row_start, block_rows)
    second_mask = local_mask(second_ancestors, row_start, block_rows)
    first_masked = first_factor * first_mask
    second_masked = second_factor * second_mask
    share_start = col_index * share_rows
    first_piece = lax.dynamic_slice_in_dim(first_masked, share_start, share_rows, 0)
    second_piece = lax.dynamic_slice_in_dim(second_masked, share_start, share_rows, 0)
    columns = known_inverse.reshape(groups * share_rows, block_rows)

    def add_piece(piece):
        return transposed_product(columns, piece)

    first_partial = add_piece(lax.all_gather(first_piece, "row", axis=0, tiled=True))
    second_partial = add_piece(lax.all_gather(second_piece, "row", axis=0, tiled=True))
    first_image = lax.psum_scatter(first_partial, "col", scatter_dimension=1, tiled=True)
    first_column = -(first_image * first_mask)
    first_full = lax.all_gather(first_column, "col", axis=1, tiled=True)
    diagonal_partial = transposed_product(first_masked, first_column)
    corner_half = lax.dynamic_slice_in_dim(first_corner, col_index * half_width, half_width, 1)
    first_diagonal = corner_half - lax.psum(diagonal_partial, "row")
    diagonal_full = lax.all_gather(first_diagonal, "col", axis=1, tiled=True)
    second_image = lax.psum_scatter(second_partial, "col", scatter_dimension=1, tiled=True)
    link_half = lax.dynamic_slice_in_dim(second_link, col_index * half_width, half_width, 1)
    second_column = -((second_image + product(first_full, link_half)) * second_mask)
    second_half = lax.dynamic_slice_in_dim(second_masked, col_index * half_width, half_width, 1)
    cross_partial = transposed_product(first_full, second_half)
    closing_partial = transposed_product(second_masked, second_column)
    cross_total, closing_total = lax.psum((cross_partial, closing_partial), "row")
    second_cross = -(cross_total + product(diagonal_full, link_half))
    second_diagonal = second_corner - closing_total - transposed_product(second_link, second_cross)
    return (first_column, first_diagonal, second_column, second_cross, second_diagonal)


def split(value):
    high = value.astype(jnp.bfloat16)
    return high, (value - high.astype(jnp.float32)).astype(jnp.bfloat16)


def dot(left, right):
    return jnp.dot(left, right, preferred_element_type=jnp.float32)


def dot3(left, right):
    (left_high, left_low), (right_high, right_low) = left, right
    return dot(left_high, right_high) + (dot(left_low, right_high) + dot(left_high, right_low))


def ring_kernel(
    n,
    known,
    factor_one,
    corner_one,
    ancestors_one,
    factor_two,
    link,
    corner_two,
    ancestors_two,
    column_one,
    diagonal_one,
    column_two,
    cross_two,
    diagonal_two,
    k_raw,
    f_raw,
    f_high,
    f_low,
    t_buf,
    own,
    link_buf,
    corner_buf,
    link_half,
    corner_half,
    corner_two_buf,
    link_split,
    half_split,
    left,
    local_sem,
    ring_send,
    ring_recv,
    pair_send,
    pair_recv,
):
    half = n // 2
    blocks = half + 1
    share = k_raw.shape[3]
    block = 2 * share
    width = link_buf.shape[0]
    hw = width // 2
    me_row = lax.axis_index("row")
    me_col = lax.axis_index("col")
    other_col = 1 - me_col

    length = n // LANES_OF_RING

    def row_at(position):
        position = lax.rem(position + n, n)
        lane = position // length
        step = position + lane * (2 * length - 1 - 2 * position)
        return step * LANES_OF_RING + lane

    lane = lax.rem(me_row, LANES_OF_RING)
    step = me_row // LANES_OF_RING
    place = step + lane * (2 * length - 1 - 2 * step)
    targets = (row_at(place + 1), row_at(place - 1))

    barrier = pltpu.get_barrier_semaphore()
    for target in targets:
        pl.semaphore_signal(barrier, inc=1, device_id={"row": target}, device_id_type=MESH)
    pl.semaphore_signal(barrier, inc=1, device_id={"col": other_col}, device_id_type=MESH)

    count = [0]

    def local(src, dst):
        copy = pltpu.make_async_copy(src, dst, local_sem.at[count[0]])
        count[0] += 1
        copy.start()
        return copy

    f_one = [local(factor_one.at[pl.ds(h * share, share)], f_raw.at[0, h, 0]) for h in range(2)]
    f_two = [local(factor_two.at[pl.ds(h * share, share)], f_raw.at[0, h, 1]) for h in range(2)]
    k_own = [local(known.at[row_at(place + i)], k_raw.at[0, me_col, i]) for i in range(blocks)]
    my_columns = pl.ds(pl.multiple_of(me_col * hw, 128), hw)
    rest = [
        local(link, link_buf),
        local(corner_one, corner_buf),
        local(link.at[:, my_columns], link_half),
        local(corner_one.at[:, my_columns], corner_half),
        local(corner_two, corner_two_buf),
    ]

    def slot(direction, t):
        return 0 if t == 0 else n - 1 if t == half else 2 * t - 1 + direction

    offsets = [0] * n
    for t in range(1, half):
        offsets[slot(0, t)], offsets[slot(1, t)] = -t, t
    offsets[n - 1] = half

    def held(at):
        return blocks if offsets[at] <= 0 else half

    def view(piece, at, which, amount):
        if piece < 2:
            return f_raw.at[at, which, piece]
        return k_raw.at[at, which, pl.ds(0, amount)]

    def pieces(direction, t):
        if t < half:
            return (0, 1, 2)
        return (0,) if direction == 0 else (1, 2)

    def ring(direction, t, piece):
        return pltpu.make_async_remote_copy(
            src_ref=view(piece, slot(direction, t - 1), me_col, held(slot(direction, t))),
            dst_ref=view(piece, slot(direction, t), me_col, held(slot(direction, t))),
            send_sem=ring_send.at[direction, t - 1, piece],
            recv_sem=ring_recv.at[direction, t - 1, piece],
            device_id={"row": targets[direction]},
            device_id_type=MESH,
        )

    def pair(at, piece, which):
        return pltpu.make_async_remote_copy(
            src_ref=view(piece, at, which, held(at)),
            dst_ref=view(piece, at, which, held(at)),
            send_sem=pair_send.at[at, piece],
            recv_sem=pair_recv.at[at, piece],
            device_id={"col": other_col},
            device_id_type=MESH,
        )

    sent = []

    def go(copy):
        copy.start()
        sent.append(copy)

    pl.semaphore_wait(barrier, 3)
    for piece, waits in ((0, f_one), (1, f_two), (2, k_own)):
        for copy in waits:
            copy.wait()
        for direction in range(2):
            go(ring(direction, 1, piece))
    go(pair(0, 2, me_col))

    for copy in rest:
        copy.wait()
    link_split[0], link_split[1] = split(link_buf[...])
    half_split[0], half_split[1] = split(link_half[...])
    corner_link = dot3(split(corner_buf[...]), (half_split[0], half_split[1]))
    cross_two[...] = -corner_link
    diagonal_one[...] = corner_half[...]
    diagonal_two[...] = corner_two_buf[...] + dot3(split(link_buf[...].T), split(corner_link))
    own[...] = jnp.zeros_like(own)

    def mask_of(ancestors, row_start):
        rows = row_start + lax.broadcasted_iota(jnp.int32, (block, ancestors.shape[1]), 0)
        same = jnp.where(rows == ancestors[...], 1.0, 0.0)
        return jnp.max(same, axis=1, keepdims=True)

    def k_block(a, b):
        i = (offsets[a] - offsets[b]) % n
        if i < half or (i == half and held(b) == blocks):
            return k_raw[b, :, i].reshape(block, block)
        return k_raw[a, :, n - i].reshape(block, block).T

    def mine(ref, start):
        return ref[:, pl.ds(pl.multiple_of(start + me_col * hw, 128), hw)]

    def mine_of(ref, rows):
        return jnp.concatenate([mine(ref.at[rows], 0), mine(ref.at[rows], width)], axis=1)

    def prepare(k):
        row_start = row_at(place + offsets[k]) * block
        first = f_raw[k, :, 0].reshape(block, width) * mask_of(ancestors_one, row_start)
        second = f_raw[k, :, 1].reshape(block, width) * mask_of(ancestors_two, row_start)
        reduced = second - dot3(split(first), (link_split[0], link_split[1]))
        rows = pl.ds(k * block, block)
        both = jnp.concatenate([first, reduced], axis=1)
        f_high[rows, :], f_low[rows, :] = split(both)
        left[k % 2, 0, :, :block], left[k % 2, 1, :, :block] = split(both.T)

    def image_of(k, slots):
        if not slots:
            return jnp.zeros((block, 2 * width), jnp.float32)
        total = None
        line_high, line_low = split(jnp.concatenate([k_block(k, j) for j in slots], axis=1))
        at, start = 0, 0
        while at < len(slots):
            upto = at
            while upto + 1 < len(slots) and slots[upto + 1] == slots[upto] + 1:
                upto += 1
            past = pl.ds(slots[at] * block, (upto + 1 - at) * block)
            columns = slice(at * block, (upto + 1) * block)
            term = dot3((line_high[:, columns], line_low[:, columns]), (f_high[past, :], f_low[past, :]))
            total = term if total is None else total + term
            at = upto + 1
        return total

    def finish(k, image):
        rows = pl.ds(k * block, block)
        my_high, my_low = mine_of(f_high, rows), mine_of(f_low, rows)
        own[...] += dot3(split(k_block(0, k)), (my_high, my_low))
        diagonal_part = dot3(split(k_block(k, k)), (my_high, my_low))
        if k == 0:
            depth = block
            right_high, right_low = split(diagonal_part)
        else:
            depth = 2 * block
            t_buf[...] = image
            left[k % 2, 0, :, block:], left[k % 2, 1, :, block:] = split(image.T)
            image_mine = jnp.concatenate([mine(t_buf, 0), mine(t_buf, width)], axis=1)
            image_high, image_low = split(image_mine + diagonal_part)
            right_high = jnp.concatenate([image_high, my_high], axis=0)
            right_low = jnp.concatenate([image_low, my_low], axis=0)
        add = dot3((left[k % 2, 0, :width, :depth], left[k % 2, 1, :width, :depth]), (right_high, right_low))
        diagonal_one[...] += add[:, :hw]
        cross_two[...] += add[:, hw:]
        diagonal_two[...] += dot3(
            (left[k % 2, 0, width:, :depth], left[k % 2, 1, width:, :depth]),
            (right_high[:, hw:], right_low[:, hw:]),
        )

    def early(k, before):
        gaps = {j: (offsets[k] - offsets[j]) % n for j in range(before)}
        return [j for j, gap in gaps.items() if gap < half or (gap == half and held(j) == blocks)]

    def take(direction, t, piece):
        ring(direction, t, piece).wait_recv()
        if piece in pieces(direction, t + 1) and t < half:
            go(ring(direction, t + 1, piece))
        go(pair(slot(direction, t), piece, me_col))

    def take_both(t, piece):
        for direction in range(2):
            if piece in pieces(direction, t):
                take(direction, t, piece)

    def paired(at, which_pieces):
        for piece in which_pieces:
            pair(at, piece, other_col).wait_recv()

    paired(0, (2,))
    prepare(0)
    finish(0, None)
    for t in range(1, half + 1):
        slots = sorted({slot(0, t), slot(1, t)})
        known = min(slots)
        take_both(t, 0)
        take_both(t, 1)
        images = {}
        for k in slots:
            paired(k, (0, 1))
            prepare(k)
            images[k] = image_of(k, early(k, known))
        take_both(t, 2)
        for k in slots:
            paired(k, (2,))
            rest_of = [j for j in range(k) if j not in early(k, known)]
            finish(k, images[k] + image_of(k, rest_of))
    first_rows = mask_of(ancestors_one, me_row * block)
    second_rows = mask_of(ancestors_two, me_row * block)
    column_one[...] = -(own[:, :hw] * first_rows)
    column_two[...] = -(own[:, hw:] * second_rows)
    for copy in sent:
        copy.wait_send()


def place_kernel(*refs):
    for source, target in zip(refs[:5], refs[5:]):
        target[...] = source[...]


def on_device_ring(
    n,
    known_inverse,
    first_factor,
    first_corner,
    first_ancestors,
    second_factor,
    second_link,
    second_corner,
    second_ancestors,
):
    groups, share, block = known_inverse.shape
    width = second_link.shape[0]
    hw = second_corner.shape[1]
    f32, bf16 = jnp.float32, jnp.bfloat16
    blocks = n // 2 + 1
    anywhere = pl.BlockSpec(memory_space=pl.ANY)
    vmem = pl.BlockSpec(memory_space=pltpu.VMEM)
    square = jax.ShapeDtypeStruct((width, hw), f32)
    column = jax.ShapeDtypeStruct((block, hw), f32)
    results = pl.pallas_call(
        functools.partial(ring_kernel, n),
        out_shape=(column, square, column, square, square),
        in_specs=[anywhere, anywhere, anywhere, vmem, anywhere, anywhere, anywhere, vmem],
        out_specs=(vmem,) * 5,
        scratch_shapes=[
            pltpu.VMEM((n, 2, blocks, share, block), f32),
            pltpu.VMEM((n, 2, 2, share, width), f32),
            pltpu.VMEM((n * block, 2 * width), bf16),
            pltpu.VMEM((n * block, 2 * width), bf16),
            pltpu.VMEM((block, 2 * width), f32),
            pltpu.VMEM((block, width), f32),
            pltpu.VMEM((width, width), f32),
            pltpu.VMEM((width, width), f32),
            pltpu.VMEM((width, hw), f32),
            pltpu.VMEM((width, hw), f32),
            pltpu.VMEM((width, hw), f32),
            pltpu.VMEM((2, width, width), bf16),
            pltpu.VMEM((2, width, hw), bf16),
            pltpu.VMEM((2, 2, 2 * width, 2 * block), bf16),
            pltpu.SemaphoreType.DMA((9 + blocks,)),
            pltpu.SemaphoreType.DMA((2, n // 2, 3)),
            pltpu.SemaphoreType.DMA((2, n // 2, 3)),
            pltpu.SemaphoreType.DMA((n, 3)),
            pltpu.SemaphoreType.DMA((n, 3)),
        ],
        compiler_params=pltpu.CompilerParams(collective_id=0, has_side_effects=True),
    )(
        known_inverse,
        first_factor,
        first_corner,
        first_ancestors.reshape(1, -1),
        second_factor,
        second_link,
        second_corner,
        second_ancestors.reshape(1, -1),
    )
    return pl.pallas_call(
        place_kernel,
        out_shape=(column, square, column, square, square),
        in_specs=[vmem] * 5,
        out_specs=(vmem,) * 5,
    )(*results)


def solution(mesh):
    def on_device(*args):
        n = mesh.shape["row"]
        groups, share, block = args[0].shape
        width = args[5].shape[0]
        held = 4 * n * block * (n * block + 4 * width)
        fits = (
            mesh.shape["col"] == 2
            and n % 4 == 0
            and groups == n
            and block == 2 * share
            and held <= VMEM_FOR_WHOLE
        )
        return on_device_ring(n, *args) if fits else on_device_collectives(*args)

    return jax.shard_map(
        on_device,
        mesh=mesh,
        in_specs=(
            P("pole", "col", "row"),
            P(("pole", "row"), None),
            P("pole", None),
            P("pole"),
            P(("pole", "row"), None),
            P("pole", None),
            P("pole", "col"),
            P("pole"),
        ),
        out_specs=(
            P(("pole", "row"), "col"),
            P("pole", "col"),
            P(("pole", "row"), "col"),
            P("pole", "col"),
            P("pole", "col"),
        ),
        check_vma=False,
    )
```
